512 devices in a mesh: rep: 8 (over z), fsdp: 64 (over y, x, core).
Axes of the slice: x: 4, y: 8, z: 8, core: 2. Of those that a mesh axis runs over, the one named last changes fastest.
Arguments:
- accumulated: bfloat16 [8, 4096, 14336], P('rep', 'fsdp'), may hold values from -16 to 16
- q_start: bfloat16 [32, 14336], P(None, 'fsdp'), may hold values from -6 to 6
Outputs:
- residual_buffer: bfloat16 [8, 4096, 14336], P('rep', 'fsdp')
- basis_f32: float32 [4096, 32], P('fsdp')
- q_factor: float32 [32, 14336], P(None, 'fsdp')
The draws below stay inside these ranges and needn't reach their ends.
All inputs are finite; a program needn't handle non-finite values.
Results may differ from the reference program's by a relative error of at most 0.0039.
Values may be sent and summed in bfloat16 or wider, within the bound.
A program may use at most 64 MiB of HBM per device.

```python
import jax
import jax.numpy as jnp
from jax import lax

COLS = 14336
RANK = 32
ITERS = 2
ROWS = 4096
N_REP = 8


def raised(drawn, own_key, source, target, shards_of, factor):
    def block_of(dim):
        return (jnp.arange(drawn.shape[dim]) // (drawn.shape[dim] // shards_of)).reshape((-1,) + (1,) * (drawn.ndim - 1 - dim))

    one_side = jax.random.permutation(own_key, shards_of)[block_of(target)]
    second = (block_of(target) + shards_of // 2) % shards_of
    return jnp.where((block_of(source) == one_side) | (block_of(source) == second), factor * drawn, drawn)


def level_of(key, extent, split, low, largest):
    level = 1.0
    for position, shards_of in split:
        heights = jax.random.uniform(jax.random.fold_in(jax.random.fold_in(key, 6), position), (shards_of,), jnp.float32, low / len(split), largest / len(split))
        level = level * jnp.repeat(jnp.exp(heights), extent[position] // shards_of).reshape((-1,) + (1,) * (len(extent) - 1 - position))
    return level


def scatter_about(own_key, shape, deviation, reach, cuts=(), dtype=jnp.bfloat16):
    values = jax.random.normal(own_key, shape, jnp.float32) * deviation
    if len(cuts) > 0:
        values = level_of(own_key, shape, cuts, -0.22, 0.18) * values
    return jnp.clip(values, min=-reach, max=reach).astype(dtype)


def gaussian_with(rng, shape, scale, bound, cuts, heavy, held_as=jnp.bfloat16):
    result = scale * jax.random.normal(rng, shape, jnp.float32)
    if cuts:
        result = result * level_of(rng, shape, cuts, -0.22, 0.18)
    return jnp.clip(raised(result, jax.random.fold_in(rng, 3), *heavy), -bound, bound).astype(held_as)


def setup_inputs(seed: int = 0) -> dict:
    seeds = jax.random.split(jax.random.key(seed), 3)
    return {
        "accumulated": gaussian_with(seeds[0], (N_REP, ROWS, COLS), 1.0, 16.0, ((0, 8), (1, 64)), (1, 2, 64, 4.0)),
        "q_start": scatter_about(seeds[1], (RANK, COLS), 1.0, 6.0, ((1, 64),)),
    }


def orthonormal(p_sum):
    gram_matrix = jnp.dot(p_sum.T, p_sum, precision=lax.Precision.HIGHEST)
    factor = jnp.linalg.cholesky(gram_matrix)
    return lax.linalg.triangular_solve(factor, p_sum, left_side=False, lower=True, transpose_a=True)

def reference(accumulated, q_start):
    right_factor = q_start
    for iteration in range(ITERS):

        def add_product(running, replica_rows):
            term = lax.dot_general(replica_rows.astype(jnp.float32), right_factor.astype(jnp.float32), (((1,), (1,)), ((), ())), preferred_element_type=jnp.float32)
            return (running + term, None)
        p_sum, unused = lax.scan(add_product, jnp.zeros((ROWS, RANK), jnp.float32), accumulated)
        basis_f32 = orthonormal(p_sum)
        basis_bf16 = basis_f32.astype(jnp.bfloat16)

        def add_columns(running, replica_rows):
            term = lax.dot_general(basis_bf16.astype(jnp.float32), replica_rows.astype(jnp.float32), (((0,), (0,)), ((), ())), preferred_element_type=jnp.float32)
            return (running + term, None)
        q_sum, unused = lax.scan(add_columns, jnp.zeros((RANK, COLS), jnp.float32), accumulated)
        q_factor = q_sum / N_REP
        right_factor = q_factor.astype(jnp.bfloat16)
    approx = lax.dot_general(basis_bf16.astype(jnp.float32), right_factor.astype(jnp.float32), (((1,), (0,)), ((), ())), preferred_element_type=jnp.float32)
    residual_buffer = lax.map(lambda replica_rows: (replica_rows.astype(jnp.float32) - approx).astype(jnp.bfloat16), accumulated)
    return (residual_buffer, basis_f32, q_factor)
```

```python
import functools

import jax
import jax.numpy as jnp
from jax import lax
from jax.experimental import pallas as pl
from jax.experimental.pallas import tpu as pltpu
from jax.sharding import PartitionSpec as P

ITERS = 2
NX = 4
NC = 2
WIDE = 256
MESH = pl.DeviceIdType.MESH
HIGHEST = lax.Precision.HIGHEST
NT = (((1,), (1,)), ((), ()))


def near_first(n):
    return sorted(range(1, n), key=lambda d: (min(d, n - d), d))


def kernel(
    nz,
    ny,
    a_hbm,
    q_ref,
    flat_ref,
    basis_ref,
    q_out,
    a_flat,
    a_pad,
    right,
    left,
    own_left,
    gram_c,
    gram_x,
    gram_y,
    w,
    w_c,
    w_x,
    w_xs,
    w_y,
    w_z,
    a_sem,
    ag_s,
    ag_r,
    p_s,
    p_r,
    g_s,
    g_r,
    w_s,
    w_r,
):
    rank, cols = q_ref.shape
    rows = a_flat.shape[0]
    z = lax.axis_index("rep")
    f = lax.axis_index("fsdp")
    c = lax.rem(f, NC)
    x = lax.rem(f // NC, NX)
    y = f // (NC * NX)
    other = 1 - c
    dxs, dys, dzs = near_first(NX), near_first(ny), near_first(nz)

    def at(yy, xx, cc):
        return (yy * NX + xx) * NC + cc

    def to(src, dst, send, recv, device):
        return pltpu.make_async_remote_copy(
            src_ref=src,
            dst_ref=dst,
            send_sem=send,
            recv_sem=recv,
            device_id=device,
            device_id_type=MESH,
        )

    x_of = [lax.rem(x + d, NX) for d in dxs]
    y_of = [lax.rem(y + d, ny) for d in dys]
    z_of = [lax.rem(z + d, nz) for d in dzs]
    x_from = [lax.rem(x + NX - d, NX) for d in dxs]
    x_peers = [(z, at(y, xx, c)) for xx in x_of]
    y_peers = [(z, at(yy, x, c)) for yy in y_of]
    z_peers = [(zz, f) for zz in z_of]
    mate = (z, at(y, x, other))

    load = pltpu.make_async_copy(a_hbm.at[0], a_flat, a_sem)
    load.start()
    barrier = pltpu.get_barrier_semaphore()
    everyone = [mate] + x_peers + y_peers + z_peers
    for peer in everyone:
        pl.semaphore_signal(barrier, inc=1, device_id=peer, device_id_type=MESH)
    right[0, c, x, y] = jnp.zeros((rank, WIDE), jnp.bfloat16)
    right[0, c, x, y, :, :cols] = q_ref[...]
    pl.semaphore_wait(barrier, len(everyone))

    def start_gather(v):
        own = right.at[v, c, x, y]
        copies = []
        for i, peer in enumerate(y_peers):
            copy = to(own, own, ag_s.at[v, i], ag_r.at[v, i], peer)
            copy.start()
            copies.append(copy)
        return copies

    def chunk(v, cc, xx):
        r = right[v, cc, xx]
        r = jnp.concatenate([r[j] for j in range(ny)], axis=1)
        return lax.dot_general(r, a_pad[cc * NX + xx], NT, preferred_element_type=jnp.float32)

    def finish_gather(v, copies, multiply=True):
        base = len(copies)
        for copy in copies:
            copy.wait_recv()
        sent, crossed, arriving = list(copies), [], []
        slab = right.at[v, c, x]
        for i, peer in enumerate(x_peers):
            copy = to(slab, slab, ag_s.at[v, base + i], ag_r.at[v, base + i], peer)
            copy.start()
            arriving.append(copy)
        base += len(arriving)

        def cross(i, xx):
            part = right.at[v, c, xx]
            copy = to(part, part, ag_s.at[v, base + i], ag_r.at[v, base + i], mate)
            copy.start()
            crossed.append(copy)

        cross(0, x)
        total = chunk(v, c, x) if multiply else None
        for i, copy in enumerate(arriving):
            copy.wait_recv()
            cross(i + 1, x_from[i])
            if multiply:
                total += chunk(v, c, x_from[i])
        for i, copy in enumerate(crossed):
            copy.wait_recv()
            if multiply:
                total += chunk(v, other, x if i == 0 else x_from[i - 1])
        for copy in sent + arriving + crossed:
            copy.wait_send()
        return total

    def exchange(buffer, slot, peers, send, recv):
        copies = []
        for i, peer in enumerate(peers):
            copy = to(buffer.at[slot], buffer.at[slot], send.at[i], recv.at[i], peer)
            copy.start()
            copies.append(copy)
        return copies

    def summed(buffer, n):
        total = buffer[0]
        for i in range(1, n):
            total += buffer[i]
        return total

    copies = start_gather(0)
    load.wait()
    for g in range(a_flat.shape[1] // (4 * cols)):
        four = a_flat[:, g * 4 * cols : (g + 1) * 4 * cols]
        for j in range(4):
            b = 4 * g + j
            bc, bx, by = b % NC, (b // NC) % NX, b // (NC * NX)
            part = jnp.concatenate(
                [four[:, j * cols : (j + 1) * cols], jnp.zeros((rows, WIDE - cols), jnp.bfloat16)],
                axis=1,
            )
            a_pad[bc * NX + bx, :, by * WIDE : (by + 1) * WIDE] = part

    half = rank // 2
    for it in range(ITERS):
        term = finish_gather(it, copies)
        left[it, z] = jnp.concatenate([term[:half], term[half:]], axis=1)
        sends = exchange(left.at[it], z, z_peers, p_s.at[it], p_r.at[it])
        for copy in sends:
            copy.wait()
        packed = summed(left.at[it], nz)
        pt = jnp.concatenate([packed[:, :rows], packed[:, rows:]], axis=0)

        below = jnp.concatenate([pt, jnp.zeros((128 - rank, rows), jnp.float32)], axis=0)
        gram = lax.dot_general(
            pt, below, NT, precision=HIGHEST, preferred_element_type=jnp.float32
        )
        gp = gram[0:8]
        for k in range(1, rank // 8):
            gp += pltpu.roll(gram[8 * k : 8 * k + 8], rank * k, 1)
        gram_c[it, c] = gp
        g_c = exchange(gram_c.at[it], c, [mate], g_s.at[it, pl.ds(0, 1)], g_r.at[it, pl.ds(0, 1)])

        hi = pt.astype(jnp.bfloat16)
        lo = (pt - hi.astype(jnp.float32)).astype(jnp.bfloat16)
        hl = jnp.concatenate([hi, lo], axis=0)

        def outer(cc, xx):
            both = lax.dot_general(
                hl,
                a_pad[cc * NX + xx],
                (((1,), (0,)), ((), ())),
                preferred_element_type=jnp.float32,
            )
            one = both[:rank] + both[rank:]
            for j in range(ny):
                w[it, cc, xx, j] = one[:, j * WIDE : (j + 1) * WIDE]

        order = x_of + [x]
        crossed = []
        for i, xx in enumerate(order):
            outer(other, xx)
            copy = to(w.at[it, other, xx], w_c.at[it, xx], w_s.at[it, i], w_r.at[it, i], mate)
            copy.start()
            crossed.append(copy)
        for copy in g_c:
            copy.wait()
        gram_x[it, x] = gram_c[it, 0] + gram_c[it, 1]
        g_x = exchange(
            gram_x.at[it], x, x_peers, g_s.at[it, pl.ds(1, NX - 1)], g_r.at[it, pl.ds(1, NX - 1)]
        )
        for xx in order:
            outer(c, xx)
        base = NX
        moved = []
        for i, xx in enumerate(x_of):
            crossed[i].wait_recv()
            w_xs[it, i] = w[it, c, xx] + w_c[it, xx]
            copy = to(
                w_xs.at[it, i], w_x.at[it, i], w_s.at[it, base + i], w_r.at[it, base + i], x_peers[i]
            )
            copy.start()
            moved.append(copy)
        base += len(moved)
        for copy in g_x:
            copy.wait()
        gram_y[it, y] = summed(gram_x.at[it], NX)
        g_y = exchange(
            gram_y.at[it], y, y_peers, g_s.at[it, pl.ds(NX, ny - 1)], g_r.at[it, pl.ds(NX, ny - 1)]
        )
        crossed[-1].wait_recv()
        w[it, c, x] = w[it, c, x] + w_c[it, x]
        for copy in moved:
            copy.wait_recv()
        for j in range(ny):
            w[it, c, x, j] = (w[it, c, x, j] + w_x[it, 0, j]) + summed(
                w_x.at[it, pl.ds(1, NX - 2), j], NX - 2
            )
        spread = []
        for i, yy in enumerate(y_of):
            copy = to(
                w.at[it, c, x, yy], w_y.at[it, i], w_s.at[it, base + i], w_r.at[it, base + i], y_peers[i]
            )
            copy.start()
            spread.append(copy)
        base += len(spread)
        for copy in g_y:
            copy.wait()
        gp = summed(gram_y.at[it], ny)
        lane = lax.broadcasted_iota(jnp.int32, (rank, 128), 1)
        row = lax.broadcasted_iota(jnp.int32, (rank, 128), 0)
        m = jnp.concatenate(
            [pltpu.roll(gp, (rank + 128 - rank * k) % 128, 1) for k in range(rank // 8)], axis=0
        )
        in_gram = (lane >= rank) & (lane < 2 * rank)
        m = jnp.where(in_gram, m, jnp.where(lane == row, 1.0, 0.0))
        scale = jnp.zeros((rank, 128), jnp.float32)
        for k in range(rank):
            pivot = m[k : k + 1, rank + k : rank + k + 1]
            column = m[:, rank + k : rank + k + 1] * (1.0 / pivot)
            scale = jnp.where(row == k, jnp.broadcast_to(lax.rsqrt(pivot), (rank, 128)), scale)
            m = m - jnp.where(row > k, column, 0.0) * m[k : k + 1, :]
        inverse = (m * scale)[:, :rank]
        for copy in spread:
            copy.wait_recv()
        w_z[it, z] = w[it, c, x, y] + summed(w_y.at[it], ny - 1)
        last = exchange(w_z.at[it], z, z_peers, w_s.at[it, pl.ds(base, nz - 1)], w_r.at[it, pl.ds(base, nz - 1)])
        if it == ITERS - 1:
            basis_ref[...] = jnp.dot(
                inverse, pt, precision=HIGHEST, preferred_element_type=jnp.float32
            )
        for copy in last:
            copy.wait_recv()
        q = jnp.dot(
            inverse, summed(w_z.at[it], nz), precision=HIGHEST, preferred_element_type=jnp.float32
        ) / nz
        right[it + 1, c, x, y] = q.astype(jnp.bfloat16)
        copies = start_gather(it + 1)
        if it == ITERS - 1:
            q_out[...] = q[:, :cols]
        for copy in crossed + moved + spread + last:
            copy.wait_send()

    finish_gather(ITERS, copies, multiply=False)
    for g in range(a_flat.shape[1] // (4 * cols)):
        parts = []
        for j in range(4):
            b = 4 * g + j
            bc, bx, by = b % NC, (b // NC) % NX, b // (NC * NX)
            parts.append(right[ITERS, bc, bx, by][:, :cols])
        flat_ref[:, g * 4 * cols : (g + 1) * 4 * cols] = jnp.concatenate(parts, axis=1)


def on_device(nz, nf, accumulated, q_start):
    rank, cols = q_start.shape
    rows = accumulated.shape[1]
    ny = nf // (NX * NC)
    bf, f32 = jnp.bfloat16, jnp.float32
    vmem = pltpu.VMEM
    dma = pltpu.SemaphoreType.DMA
    n_ag = ny - 1 + NX - 1 + NX
    n_g = 1 + NX - 1 + ny - 1
    n_w = NX + NX - 1 + ny - 1 + nz - 1
    flat, basis_t, q_factor = pl.pallas_call(
        functools.partial(kernel, nz, ny),
        out_shape=(
            jax.ShapeDtypeStruct((rank, nf * cols), bf),
            jax.ShapeDtypeStruct((rank, rows), f32),
            jax.ShapeDtypeStruct((rank, cols), f32),
        ),
        in_specs=[pl.BlockSpec(memory_space=pl.ANY), pl.BlockSpec(memory_space=vmem)],
        out_specs=[pl.BlockSpec(memory_space=vmem)] * 3,
        scratch_shapes=[
            vmem((rows, nf * cols), bf),
            vmem((NC * NX, rows, ny * WIDE), bf),
            vmem((ITERS + 1, NC, NX, ny, rank, WIDE), bf),
            vmem((ITERS, nz, rank // 2, 2 * rows), f32),
            vmem((8, 128), f32),
            vmem((ITERS, NC, 8, 128), f32),
            vmem((ITERS, NX, 8, 128), f32),
            vmem((ITERS, ny, 8, 128), f32),
            vmem((ITERS, NC, NX, ny, rank, WIDE), f32),
            vmem((ITERS, NX, ny, rank, WIDE), f32),
            vmem((ITERS, NX - 1, ny, rank, WIDE), f32),
            vmem((ITERS, NX - 1, ny, rank, WIDE), f32),
            vmem((ITERS, ny - 1, rank, WIDE), f32),
            vmem((ITERS, nz, rank, WIDE), f32),
            dma,
            dma((ITERS + 1, n_ag)),
            dma((ITERS + 1, n_ag)),
            dma((ITERS, nz - 1)),
            dma((ITERS, nz - 1)),
            dma((ITERS, n_g)),
            dma((ITERS, n_g)),
            dma((ITERS, n_w)),
            dma((ITERS, n_w)),
        ],
        compiler_params=pltpu.CompilerParams(
            collective_id=0, has_side_effects=True, vmem_limit_bytes=48 * 1024 * 1024
        ),
    )(accumulated, q_start)
    approx = jnp.dot(basis_t.T.astype(bf), flat, preferred_element_type=f32)
    residual = (accumulated[0].astype(f32) - approx).astype(bf)[None]
    return residual, basis_t.T, q_factor


def solution(mesh):
    nz, nf = mesh.shape["rep"], mesh.shape["fsdp"]
    in_specs = (P("rep", "fsdp", None), P(None, "fsdp"))
    out_specs = (P("rep", "fsdp", None), P("fsdp", None), P(None, "fsdp"))
    return jax.shard_map(
        functools.partial(on_device, nz, nf),
        mesh=mesh,
        in_specs=in_specs,
        out_specs=out_specs,
        check_vma=False,
    )
```
